32 devices in a mesh: blk: 8 (over z, y), dp: 4 (over x, core).
Axes of the slice: x: 2, y: 2, z: 4, core: 2. Of those that a mesh axis runs over, the one named last changes fastest.
Arguments:
- memory: float32 [65536, 172], P(('blk', 'dp')), may hold values from -3 to 3
- src: int32 [2, 4096], P(None, ('blk', 'dp')), may hold values from 0 to 2047, as said below
- dst: int32 [2, 4096], P(None, ('blk', 'dp')), may hold values from 0 to 2047, as said below
- negative: int32 [2, 4096], P(None, ('blk', 'dp')), may hold values from 0 to 2047
- event_time: int32 [2, 4096], P(None, ('blk', 'dp')), may hold values from 0 to 1023
- neighbours: int32 [2, 10, 12288], P(None, None, ('blk', 'dp')), may hold values from 0 to 2047
- neighbour_time: int32 [2, 10, 12288], P(None, None, ('blk', 'dp')), may hold values from 0 to 1023
- time_omega: float32 [100], replicated, may hold values from 0.001 to 1
- w_input: float32 [444, 516], replicated, may hold values from -0.25 to 0.25
- w_hidden: float32 [172, 516], replicated, may hold values from -0.4375 to 0.4375
- gru_bias: float32 [2, 516], replicated, may hold values from -3 to 3
- w_query: float32 [172, 172], replicated, may hold values from -0.4807515 to 0.4807515
- w_keyval: float32 [272, 344], replicated, may hold values from -0.7508627 to 0.7508627
- w_decode: float32 [172], replicated, may hold values from -0.875 to 0.875
Outputs:
- memory_out: float32 [65536, 172], P(('blk', 'dp'))
- losses: float32 [2], replicated
- w_input_out: float32 [444, 516], replicated
- w_hidden_out: float32 [172, 516], replicated
- gru_bias_out: float32 [2, 516], replicated
- w_query_out: float32 [172, 172], replicated
- w_keyval_out: float32 [272, 344], replicated
- w_decode_out: float32 [172], replicated
The draws below stay inside these ranges and needn't reach their ends.
Inputs may be any that keep to these rules, and one draw needn't show every extreme that they name: In each step and event block, the 128 src and 128 dst entries are 256 different rows. `dst`: different from every src entry of the same step and event block, and from each other.
All inputs are finite; a program needn't handle non-finite values.
Results may differ from the reference program's by a relative error of at most 0.00012.
Values sent between devices are 32-bit elements; how exact they have to be, the bound alone decides.
No kernel may reach another device: no remote copies, remote signals or barrier semaphores. Data moves between devices by JAX's collectives and lax.ppermute only.
A program may use at most 128 MiB of HBM per device.

```python
import math
import jax
import jax.numpy as jnp
from jax import lax

MEM = 172
TD = 100
HEADS = 2
NBR = 10
E_DEV = 128
ROWS_DEV = 2048
STEPS = 2
BUCKETS = 1024
MSG = 444
KIN = 272
EVENTS = 4096
NODES = 65536
N_BLK = 8
N_DP = 4


def pick_rows(key):
    blocks = EVENTS // E_DEV
    keys = jax.random.split(jax.random.fold_in(key, 17), STEPS * blocks)
    perms = jax.vmap(lambda k: jax.random.permutation(k, ROWS_DEV))(keys)
    return perms[:, :2 * E_DEV].astype(jnp.int32)


def draw_src(key, part):
    rows = pick_rows(key)
    return rows[:, :E_DEV].reshape(STEPS, EVENTS)


def draw_dst(key, part):
    rows = pick_rows(key)
    return rows[:, E_DEV:].reshape(STEPS, EVENTS)


def draw_memory(key, part):
    values = jnp.clip(0.5 * jax.random.normal(jax.random.fold_in(key, 3), (NODES, MEM), jnp.float32), -3.0, 3.0)
    return values


def draw_w_query(key, part):
    values = jnp.clip(jax.random.normal(jax.random.fold_in(key, 7), (MEM, MEM), jnp.float32), -6.0, 6.0) / jnp.sqrt(jnp.float32(MEM))
    return values


def draw_w_keyval(key, part):
    values = jnp.clip(jax.random.normal(jax.random.fold_in(key, 8), (KIN, 2 * MEM), jnp.float32), -6.0, 6.0) / jnp.sqrt(jnp.float32(KIN))
    column = jnp.arange(2 * MEM)
    values = values * jnp.where(column < MEM, 1.0, 2.0).astype(jnp.float32)[None, :]
    return values


def with_ends(values, own_key, least, top_value):
    spot = [jax.random.randint(jax.random.fold_in(own_key, axis), (), 0, length) for axis, length in enumerate(values.shape)]
    longest = values.shape.index(max(values.shape))
    next_to = spot[:longest] + [(spot[longest] + 1) % values.shape[longest]] + spot[longest + 1:]
    return values.at[tuple(spot)].set(least).at[tuple(next_to)].set(top_value)


def bell_draw(stream_key, dims, spread, most, held_as=jnp.bfloat16):
    entries = jax.random.normal(stream_key, dims, jnp.float32) * spread
    return jnp.minimum(jnp.maximum(entries, -most), most).astype(held_as)


def setup_inputs(seed: int = 0) -> dict:
    key_of = jax.random.split(jax.random.key(seed), 15)
    memory = draw_memory(jax.random.fold_in(key_of[14], 71), 0)
    src = draw_src(jax.random.fold_in(key_of[14], 71), 0)
    dst = draw_dst(jax.random.fold_in(key_of[14], 71), 0)
    negative = with_ends(jax.random.randint(key_of[3], (STEPS, EVENTS), 0, ROWS_DEV), jax.random.fold_in(key_of[3], 1), 0, ROWS_DEV - 1).astype(jnp.int32)
    event_time = with_ends(jax.random.randint(key_of[4], (STEPS, EVENTS), 0, BUCKETS), jax.random.fold_in(key_of[4], 1), 0, BUCKETS - 1).astype(jnp.int32)
    neighbours = with_ends(jax.random.randint(key_of[5], (STEPS, NBR, 3 * EVENTS), 0, ROWS_DEV), jax.random.fold_in(key_of[5], 1), 0, ROWS_DEV - 1).astype(jnp.int32)
    neighbour_time = with_ends(jax.random.randint(key_of[6], (STEPS, NBR, 3 * EVENTS), 0, BUCKETS), jax.random.fold_in(key_of[6], 1), 0, BUCKETS - 1).astype(jnp.int32)
    time_omega = jnp.clip(jnp.exp(jax.random.uniform(key_of[7], (TD,), jnp.float32, math.log(0.001), math.log(1.0))), 0.001, 1.0)
    w_input = bell_draw(key_of[8], (MSG, 3 * MEM), MSG ** -0.5, 0.25, jnp.float32)
    w_hidden = bell_draw(key_of[9], (MEM, 3 * MEM), MEM ** -0.5, 0.4375, jnp.float32)
    gru_bias = bell_draw(key_of[10], (2, 3 * MEM), 0.5, 3.0, jnp.float32)
    w_query = draw_w_query(jax.random.fold_in(key_of[14], 71), 0)
    w_keyval = draw_w_keyval(jax.random.fold_in(key_of[14], 71), 0)
    w_decode = bell_draw(key_of[13], (MEM,), (MEM // 4) ** -0.5, 0.875, jnp.float32)
    return dict(memory=memory, src=src, dst=dst, negative=negative, event_time=event_time, neighbours=neighbours, neighbour_time=neighbour_time, time_omega=time_omega, w_input=w_input, w_hidden=w_hidden, gru_bias=gru_bias, w_query=w_query, w_keyval=w_keyval, w_decode=w_decode)


rate = 0.25
exact = lax.Precision.HIGHEST

def step_loss(params, memory, src_ids, dst_ids, neg_ids, times, nbr_ids, nbr_times, omega, count):
    w_input, w_hidden, gru_bias, w_query, w_keyval, w_decode = params
    width = memory.shape[1]
    events = src_ids.shape[0]
    h_src = memory[src_ids]
    h_dst = memory[dst_ids]
    stamp = times.astype(jnp.float32)
    tenc = jnp.cos(stamp[:, None] * omega[None, :])
    inputs = jnp.concatenate([jnp.concatenate([h_src, h_dst, tenc], 1), jnp.concatenate([h_dst, h_src, tenc], 1)], 0)
    hidden = jnp.concatenate([h_src, h_dst], 0)
    gate_in = jnp.dot(inputs, w_input, precision=exact, preferred_element_type=jnp.float32) + gru_bias[0]
    gate_hid = jnp.dot(hidden, w_hidden, precision=exact, preferred_element_type=jnp.float32) + gru_bias[1]
    reset = jax.nn.sigmoid(gate_in[:, :width] + gate_hid[:, :width])
    update = jax.nn.sigmoid(gate_in[:, width:2 * width] + gate_hid[:, width:2 * width])
    cand = jnp.tanh(gate_in[:, 2 * width:] + reset * gate_hid[:, 2 * width:])
    fresh = (1.0 - update) * cand + update * hidden
    touched = jnp.concatenate([src_ids, dst_ids], 0)
    updated = memory.at[touched].set(fresh)
    query_ids = jnp.concatenate([src_ids, dst_ids, neg_ids], 0)
    query_mem = updated[query_ids]
    rows = query_ids.shape[0]
    row_time = jnp.concatenate([stamp, stamp, stamp], 0)
    nbr_mem = updated[nbr_ids]
    delta = row_time[None, :] - nbr_times.astype(jnp.float32)
    nenc = jnp.cos(delta[:, :, None] * omega[None, None, :])
    key_in = jnp.concatenate([nbr_mem, nenc], 2)
    count_nbr = key_in.shape[0]
    keyval = jnp.dot(key_in.reshape(count_nbr * rows, -1), w_keyval, precision=exact, preferred_element_type=jnp.float32)
    keyval = keyval.reshape(count_nbr, rows, 2 * width)
    query = jnp.dot(query_mem, w_query, precision=exact, preferred_element_type=jnp.float32)
    head_size = width // HEADS
    keys = keyval[:, :, :width].reshape(count_nbr, rows, HEADS, head_size)
    values = keyval[:, :, width:].reshape(count_nbr, rows, HEADS, head_size)
    query = query.reshape(rows, HEADS, head_size)
    scores = lax.optimization_barrier(jnp.sum(keys * query[None], -1)) / jnp.sqrt(jnp.float32(head_size))
    top = lax.optimization_barrier(jnp.max(scores, 0, keepdims=True))
    probs = jnp.exp(scores - top)
    probs = probs / lax.optimization_barrier(jnp.sum(probs, 0, keepdims=True))
    attn = lax.optimization_barrier(jnp.sum(probs[:, :, :, None] * values, 0)).reshape(rows, width)
    embed = query_mem + attn
    e_src = embed[:events]
    e_dst = embed[events:2 * events]
    e_neg = embed[2 * events:]
    pos = lax.optimization_barrier(jnp.sum(e_src * e_dst * w_decode[None, :], 1))
    neg = lax.optimization_barrier(jnp.sum(e_src * e_neg * w_decode[None, :], 1))
    loss = jnp.sum(jax.nn.softplus(-pos) + jax.nn.softplus(neg)) / count
    return (loss, updated)

def reference(memory, src, dst, negative, event_time, neighbours, neighbour_time, time_omega, w_input, w_hidden, gru_bias, w_query, w_keyval, w_decode):
    groups = N_BLK * N_DP
    count = jnp.float32(E_DEV * groups)
    params = (w_input, w_hidden, gru_bias, w_query, w_keyval, w_decode)
    state = memory.reshape(groups, ROWS_DEV, MEM)
    losses = []
    for step in range(STEPS):
        src_b = src[step].reshape(groups, E_DEV)
        dst_b = dst[step].reshape(groups, E_DEV)
        neg_b = negative[step].reshape(groups, E_DEV)
        time_b = event_time[step].reshape(groups, E_DEV)
        nbr_b = jnp.transpose(neighbours[step].reshape(NBR, groups, 3 * E_DEV), (1, 0, 2))
        ntime_b = jnp.transpose(neighbour_time[step].reshape(NBR, groups, 3 * E_DEV), (1, 0, 2))

        def one_block(carry, xs):
            mem_g, s_g, d_g, n_g, t_g, nb_g, nt_g = xs
            fn = lambda p: step_loss(p, mem_g, s_g, d_g, n_g, t_g, nb_g, nt_g, time_omega, count)
            loss, back, updated = jax.vjp(fn, params, has_aux=True)
            grads = back(jnp.float32(1.0))[0]
            sums, total = carry
            sums = tuple((a + b for a, b in zip(sums, grads)))
            return ((sums, total + loss), updated)
        zeros = tuple((jnp.zeros_like(p) for p in params))
        (sums, total), new_state = lax.scan(one_block, (zeros, jnp.float32(0.0)), (state, src_b, dst_b, neg_b, time_b, nbr_b, ntime_b))
        params = tuple((p - rate * g for p, g in zip(params, sums)))
        losses.append(total)
        new_state = new_state.reshape(N_BLK, N_DP, ROWS_DEV, MEM)
        state = jnp.roll(new_state, 1, axis=0).reshape(groups, ROWS_DEV, MEM)
    memory_out = state.reshape(groups * ROWS_DEV, MEM)
    return (memory_out, jnp.stack(losses), params[0], params[1], params[2], params[3], params[4], params[5])
```

```python
import jax
import jax.numpy as jnp
from jax import lax
from jax.experimental import pallas as pl
from jax.experimental.pallas import tpu as pltpu
from jax.sharding import PartitionSpec as P

HEADS = 2
STEPS = 2
AXES = ("blk", "dp")

rate = 0.25


def passed_along(shard, axis, by):
    devices = lax.axis_size(axis)
    return lax.ppermute(shard, axis, [(i, (i + by) % devices) for i in range(devices)])


def split2(x):
    hi = x.astype(jnp.bfloat16)
    lo = (x - hi.astype(jnp.float32)).astype(jnp.bfloat16)
    return hi, lo


def raw_dot(a, b, dims):
    return lax.dot_general(a, b, (dims, ((), ())), preferred_element_type=jnp.float32)


NN = ((1,), (0,))
NT = ((1,), (1,))
TN = ((0,), (0,))


def dot3(a, b, dims=NN):
    return raw_dot(a[0], b[0], dims) + (raw_dot(a[0], b[1], dims) + raw_dot(a[1], b[0], dims))


def dot_exact_left(a, b, dims=NN):
    return raw_dot(a, b[0], dims) + raw_dot(a, b[1], dims)


def dot_exact_right(a, b, dims=NN):
    return raw_dot(a[0], b, dims) + raw_dot(a[1], b, dims)


def up8(n):
    return -(-n // 8) * 8


class Packing:
    def __init__(self, width, tdim, devices):
        self.width, self.tdim = width, tdim
        self.a, self.b = up8(width), up8(tdim)
        self.b0 = 12 * self.a
        self.c0 = self.b0 + 5 * self.b
        unit = 8 * devices
        self.rows = -(-(self.c0 + 8) // unit) * unit

    def sec_a(self, i):
        return slice(i * self.a, i * self.a + self.width)

    def sec_b(self, i):
        return slice(self.b0 + i * self.b, self.b0 + i * self.b + self.tdim)

    def row(self, i):
        return slice(self.c0 + i, self.c0 + i + 1)

    def pack(self, w_input, w_hidden, gru_bias, w_query, w_keyval, w_decode):
        w = self.width
        gates = [slice(g * w, (g + 1) * w) for g in range(3)]
        a = [w_input[:w, s] for s in gates] + [w_input[w : 2 * w, s] for s in gates]
        a += [w_hidden[:, s] for s in gates] + [w_query, w_keyval[:w, :w], w_keyval[:w, w:]]
        b = [w_input[2 * w :, s] for s in gates] + [w_keyval[w:, :w], w_keyval[w:, w:]]
        pads = [jnp.pad(x, ((0, self.a - w), (0, 0))) for x in a]
        pads += [jnp.pad(x, ((0, self.b - self.tdim), (0, 0))) for x in b]
        tail = jnp.concatenate([gru_bias.reshape(6, w), w_decode[None, :]], 0)
        pads.append(jnp.pad(tail, ((0, self.rows - self.c0 - 7), (0, 0))))
        return jnp.concatenate(pads, 0)

    def unpack(self, p):
        a = [p[self.sec_a(i)] for i in range(12)]
        b = [p[self.sec_b(i)] for i in range(5)]
        w_input = jnp.concatenate(
            [jnp.concatenate([a[g], a[3 + g], b[g]], 0) for g in range(3)], 1
        )
        w_hidden = jnp.concatenate(a[6:9], 1)
        w_keyval = jnp.concatenate(
            [jnp.concatenate([a[10], b[3]], 0), jnp.concatenate([a[11], b[4]], 0)], 1
        )
        bias = p[self.c0 : self.c0 + 6].reshape(2, 3 * self.width)
        return w_input, w_hidden, bias, a[9], w_keyval, p[self.c0 + 6]


def gru_kernel(pk, h_ref, h2_ref, e2_ref, p_ref, fresh_ref, save_ref):
    h = h_ref[...]
    hs, h2s, es = split2(h), split2(h2_ref[...]), split2(e2_ref[...])

    def gates(g):
        gi = dot3(hs, split2(p_ref[pk.sec_a(g), :]))
        gi += dot3(h2s, split2(p_ref[pk.sec_a(3 + g), :]))
        gi += dot3(es, split2(p_ref[pk.sec_b(g), :]))
        gi += p_ref[pk.row(g), :]
        gh = dot3(hs, split2(p_ref[pk.sec_a(6 + g), :])) + p_ref[pk.row(3 + g), :]
        return gi, gh

    gi, gh = gates(0)
    reset = jax.nn.sigmoid(gi + gh)
    gi, gh = gates(1)
    update = jax.nn.sigmoid(gi + gh)
    gi, gh = gates(2)
    cand = jnp.tanh(gi + reset * gh)
    fresh_ref[...] = (1.0 - update) * cand + update * h
    save_ref[0] = reset
    save_ref[1] = update
    save_ref[2] = cand
    save_ref[3] = gh


def softplus(x):
    return jnp.maximum(x, 0.0) + jnp.log1p(jnp.exp(-jnp.abs(x)))


def attn_kernel(
    pk, inv_count, h_ref, h2_ref, e2_ref, fresh_ref, save_ref, negm_ref, nbrm_ref, nenc_ref,
    touched_ref, negid_ref, nbrid_ref, p_ref, g_ref, nm_ref, k_ref, v_ref, s_ref,
):
    n_nbr, rows, width = nbrm_ref.shape
    both = h_ref.shape[0]
    events = both // 2
    head = width // HEADS
    inv_root = 1.0 / (head**0.5)
    bf = jnp.bfloat16
    touched = touched_ref[...]

    def onehot(ids):
        hit = (ids == touched).astype(jnp.float32)
        return hit.astype(bf), 1.0 - jnp.max(hit, axis=1, keepdims=True)

    ri = lax.broadcasted_iota(jnp.int32, (width, width), 0) // head
    ci = lax.broadcasted_iota(jnp.int32, (width, width), 1) // head
    same = (ri == ci).astype(jnp.float32).astype(bf)

    def head_sum(x):
        return dot_exact_right(split2(x), same)

    g_ref[...] = jnp.zeros(g_ref.shape, jnp.float32)
    fresh = fresh_ref[...]
    fs = split2(fresh)
    o_neg, keep = onehot(negid_ref[...])
    neg_mem = negm_ref[...] * keep + dot_exact_left(o_neg, fs)
    qmem = jnp.concatenate([fresh, neg_mem], 0)
    qms = split2(qmem)
    wq = split2(p_ref[pk.sec_a(9), :])
    query = dot3(qms, wq) * inv_root
    wk1 = split2(p_ref[pk.sec_a(10), :])
    wv1 = split2(p_ref[pk.sec_a(11), :])
    wk2 = split2(p_ref[pk.sec_b(3), :])
    wv2 = split2(p_ref[pk.sec_b(4), :])

    top = None
    for j in range(n_nbr):
        o_j, keep = onehot(nbrid_ref[j])
        mem = nbrm_ref[j] * keep + dot_exact_left(o_j, fs)
        nm_ref[j] = mem
        ms = split2(mem)
        ns = split2(nenc_ref[j])
        key = dot3(ms, wk1) + dot3(ns, wk2)
        k_ref[j] = key
        v_ref[j] = dot3(ms, wv1) + dot3(ns, wv2)
        score = head_sum(key * query)
        s_ref[j] = score
        top = score if top is None else jnp.maximum(top, score)
    den = jnp.zeros_like(top)
    acc = jnp.zeros_like(top)
    for j in range(n_nbr):
        prob = jnp.exp(s_ref[j] - top)
        s_ref[j] = prob
        den += prob
        acc += prob * v_ref[j]
    inv_den = 1.0 / den
    attn = acc * inv_den
    embed = qmem + attn
    e_s, e_d, e_n = embed[:events], embed[events:both], embed[both:]
    w_dec = p_ref[pk.row(6), :]
    sw = e_s * w_dec
    pos = jnp.sum(sw * e_d, axis=1, keepdims=True)
    neg = jnp.sum(sw * e_n, axis=1, keepdims=True)
    loss = jnp.sum(softplus(-pos) + softplus(neg), axis=0, keepdims=True) * inv_count
    d_pos = -jax.nn.sigmoid(-pos) * inv_count
    d_neg = jax.nn.sigmoid(neg) * inv_count
    mix = d_pos * e_d + d_neg * e_n
    g_ref[pk.row(6), :] = jnp.sum(e_s * mix, axis=0, keepdims=True)
    g_ref[pk.row(7), :] = jnp.broadcast_to(loss, (1, width))
    d_embed = jnp.concatenate([mix * w_dec, d_pos * sw, d_neg * sw], 0)

    mean_dp = head_sum(d_embed * attn)
    d_query = jnp.zeros_like(query)
    r_k = jnp.zeros((both, width), jnp.float32)
    r_v = jnp.zeros((both, width), jnp.float32)
    for j in range(n_nbr):
        prob = s_ref[j] * inv_den
        d_score = prob * (head_sum(d_embed * v_ref[j]) - mean_dp)
        d_query += d_score * k_ref[j]
        d_key = split2(d_score * query)
        d_val = split2(prob * d_embed)
        ms = split2(nm_ref[j])
        ns = split2(nenc_ref[j])
        g_ref[pk.sec_a(10), :] += dot3(ms, d_key, TN)
        g_ref[pk.sec_a(11), :] += dot3(ms, d_val, TN)
        g_ref[pk.sec_b(3), :] += dot3(ns, d_key, TN)
        g_ref[pk.sec_b(4), :] += dot3(ns, d_val, TN)
        o_j = (nbrid_ref[j] == touched).astype(jnp.float32).astype(bf)
        r_k += dot_exact_left(o_j, d_key, TN)
        r_v += dot_exact_left(o_j, d_val, TN)
    dqs = split2(d_query * inv_root)
    g_ref[pk.sec_a(9), :] = dot3(qms, dqs, TN)
    d_qmem = d_embed + dot3(dqs, wq, NT)
    d_fresh = d_qmem[:both] + dot_exact_left(o_neg, split2(d_qmem[both:]), TN)
    d_fresh += dot3(split2(r_k), wk1, NT) + dot3(split2(r_v), wv1, NT)

    h = h_ref[...]
    reset, update, cand, gh_n = save_ref[0], save_ref[1], save_ref[2], save_ref[3]
    d_z = d_fresh * (h - cand) * update * (1.0 - update)
    d_n = d_fresh * (1.0 - update) * (1.0 - cand * cand)
    d_hn = d_n * reset
    d_r = d_n * gh_n * reset * (1.0 - reset)
    hs, h2s, es = split2(h), split2(h2_ref[...]), split2(e2_ref[...])
    for g, d in enumerate((d_r, d_z, d_n)):
        ds = split2(d)
        by_h = dot3(hs, ds, TN)
        g_ref[pk.sec_a(g), :] = by_h
        g_ref[pk.sec_a(3 + g), :] = dot3(h2s, ds, TN)
        g_ref[pk.sec_b(g), :] = dot3(es, ds, TN)
        d_bias = jnp.sum(d, axis=0, keepdims=True)
        g_ref[pk.row(g), :] = d_bias
        if g < 2:
            g_ref[pk.sec_a(6 + g), :] = by_h
            g_ref[pk.row(3 + g), :] = d_bias
        else:
            g_ref[pk.sec_a(8), :] = dot3(hs, split2(d_hn), TN)
            g_ref[pk.row(5), :] = jnp.sum(d_hn, axis=0, keepdims=True)


VMEM_LIMIT = 56 * 1024 * 1024


def gru(pk, h, h2, e2, p):
    shape = jax.ShapeDtypeStruct(h.shape, jnp.float32)
    saved = jax.ShapeDtypeStruct((4,) + h.shape, jnp.float32)
    return pl.pallas_call(
        lambda *refs: gru_kernel(pk, *refs),
        out_shape=(shape, saved),
        compiler_params=pltpu.CompilerParams(vmem_limit_bytes=VMEM_LIMIT),
        name="gru",
    )(h, h2, e2, p)


def attention(pk, inv_count, *args):
    big = pltpu.VMEM(args[6].shape, jnp.float32)
    return pl.pallas_call(
        lambda *refs: attn_kernel(pk, inv_count, *refs),
        out_shape=jax.ShapeDtypeStruct(args[-1].shape, jnp.float32),
        scratch_shapes=[big] * 4,
        compiler_params=pltpu.CompilerParams(vmem_limit_bytes=VMEM_LIMIT),
        name="attention",
    )(*args)


def summed(grads):
    return lax.psum(grads, AXES)


def on_device(
    memory,
    src,
    dst,
    negative,
    event_time,
    neighbours,
    neighbour_time,
    time_omega,
    *weights,
):
    width, tdim = memory.shape[1], time_omega.shape[0]
    n_dev = lax.axis_size("blk") * lax.axis_size("dp")
    pk = Packing(width, tdim, n_dev)
    inv_count = 1.0 / float(src.shape[1] * n_dev)
    params = pk.pack(*weights)
    losses = []
    for step in range(STEPS):
        events = src.shape[1]
        n_nbr, rows = neighbours.shape[1:]
        touched = jnp.concatenate([src[step], dst[step]], 0)
        h = memory.at[touched].get(mode="promise_in_bounds")
        h2 = jnp.concatenate([h[events:], h[:events]], 0)
        negm = memory.at[negative[step]].get(mode="promise_in_bounds")
        nbrm = memory.at[neighbours[step].reshape(-1)].get(mode="promise_in_bounds")
        nbrm = nbrm.reshape(n_nbr, rows, width)
        stamp = event_time[step].astype(jnp.float32)
        tenc = jnp.cos(stamp[:, None] * time_omega[None, :])
        e2 = jnp.concatenate([tenc, tenc], 0)
        row_time = jnp.concatenate([stamp, stamp, stamp], 0)
        delta = row_time[None, :] - neighbour_time[step].astype(jnp.float32)
        nenc = jnp.cos(delta[:, :, None] * time_omega[None, None, :])
        fresh, saved = gru(pk, h, h2, e2, params)
        updated = memory.at[touched].set(
            fresh, mode="promise_in_bounds", unique_indices=True
        )
        memory = passed_along(updated, "blk", 1)
        grads = attention(
            pk, inv_count, h, h2, e2, fresh, saved, negm, nbrm, nenc,
            touched[None, :], negative[step][:, None], neighbours[step][:, :, None], params,
        )
        sums = summed(grads)
        losses.append(sums[pk.c0 + 7, 0])
        params = params - rate * sums
    return (memory, jnp.stack(losses)) + pk.unpack(params)


def solution(mesh):
    rows = P(("blk", "dp"), None)
    ids = P(None, ("blk", "dp"))
    nbrs = P(None, None, ("blk", "dp"))
    return jax.shard_map(
        on_device,
        mesh=mesh,
        in_specs=(rows, ids, ids, ids, ids, nbrs, nbrs) + (P(),) * 7,
        out_specs=(rows,) + (P(),) * 7,
        check_vma=False,
    )
```
